256 devices in a mesh: row: 32 (over z, x_hi, core), col: 8 (over x_lo, y).
Axes of the slice: x: 4 (x_hi: 2, x_lo: 2; x = x_hi * 2 + x_lo), y: 4, z: 8, core: 2. Of those that a mesh axis runs over, the one named last changes fastest.
Arguments:
- teacher_hidden: bfloat16 [1024, 4608], P('row', 'col'), as said below
- student_hidden: bfloat16 [1024, 3584], P('row', 'col'), as said below
- teacher_embed: bfloat16 [131072, 4608], P(('row', 'col')), may hold values from -0.4861359 to 0.4861359
- student_embed: bfloat16 [131072, 3584], P(('row', 'col')), may hold values from -0.5512263 to 0.5512263
Outputs:
- divergence: float32 [1024], P(('row', 'col'))
- mean_divergence: float32 [], replicated
The draws below stay inside these ranges and needn't reach their ends.
Inputs may be any that keep to these rules, and one draw needn't show every extreme that they name: `teacher_hidden`: entries of order one; a few rows may be far larger. `student_hidden`: entries of order one; a few rows may be far larger.
All inputs are finite; a program needn't handle non-finite values.
Results may differ from the reference program's by a relative error of at most 0.0003.
Values may be sent and summed in bfloat16 or wider, within the bound.
No kernel may reach another device: no remote copies, remote signals or barrier semaphores. Data moves between devices by JAX's collectives and lax.ppermute only.
A program may use at most 64 MiB of HBM per device.

```python
import math
import jax
import jax.numpy as jnp
from jax import lax

D_T = 4608
D_S = 3584
VOCAB_DEV = 512
TOKENS = 1024
VOCAB = 131072
N_COL = 8


def build_table(key, width, model_tag):
    table_key = jax.random.fold_in(key, 11 + model_tag)
    slope = 0.6 + 1.2 * jnp.arange(VOCAB, dtype=jnp.float32) / VOCAB
    entries = jnp.clip(jax.random.normal(table_key, (VOCAB, width), jnp.float32), -6.0, 6.0)
    table = entries * slope[:, None] * (3.0 / math.sqrt(width))
    return table


def build_states(key, width, model_tag):
    state_key = jax.random.fold_in(key, 23 + model_tag)
    key_values = jax.random.fold_in(state_key, 0)
    states = jnp.clip(jax.random.normal(key_values, (TOKENS, width), jnp.float32), -6.0, 6.0)
    return states


def draw_teacher_hidden(key, part):
    return build_states(key, D_T, 0).astype(jnp.bfloat16)


def draw_student_hidden(key, part):
    return build_states(key, D_S, 1).astype(jnp.bfloat16)


def draw_teacher_embed(key, part):
    return build_table(key, D_T, 0).astype(jnp.bfloat16)


def draw_student_embed(key, part):
    return build_table(key, D_S, 1).astype(jnp.bfloat16)


def setup_inputs(seed: int = 0) -> dict:
    arg_keys = jax.random.split(jax.random.key(seed), 5)
    return {
        "teacher_hidden": draw_teacher_hidden(jax.random.fold_in(arg_keys[4], 71), 0),
        "student_hidden": draw_student_hidden(jax.random.fold_in(arg_keys[4], 71), 0),
        "teacher_embed": draw_teacher_embed(jax.random.fold_in(arg_keys[4], 71), 0),
        "student_embed": draw_student_embed(jax.random.fold_in(arg_keys[4], 71), 0),
    }


def reference(teacher_hidden, student_hidden, teacher_embed, student_embed):
    width_block = VOCAB_DEV * N_COL
    blocks = VOCAB // width_block
    teacher_blocks = teacher_embed.reshape(blocks, width_block, D_T)
    student_blocks = student_embed.reshape(blocks, width_block, D_S)

    def advance(running, tables):
        top_teacher, sum_teacher, cross_term, top_student, sum_student = running
        logit_teacher = jnp.dot(teacher_hidden, tables[0].T, preferred_element_type=jnp.float32)
        logit_student = jnp.dot(student_hidden, tables[1].T, preferred_element_type=jnp.float32)
        high_teacher = jnp.maximum(top_teacher, jnp.max(logit_teacher, 1))
        high_student = jnp.maximum(top_student, jnp.max(logit_student, 1))
        weights = jnp.exp(logit_teacher - high_teacher[:, None])
        decay_teacher = jnp.exp(top_teacher - high_teacher)
        decay_student = jnp.exp(top_student - high_student)
        sum_teacher = sum_teacher * decay_teacher + jnp.sum(weights, 1)
        cross_term = cross_term * decay_teacher + jnp.sum(weights * (logit_teacher - logit_student), 1)
        sum_student = sum_student * decay_student + jnp.sum(jnp.exp(logit_student - high_student[:, None]), 1)
        return (high_teacher, sum_teacher, cross_term, high_student, sum_student), None

    lowest = jnp.full((TOKENS,), -1e30, jnp.float32)
    nothing = jnp.zeros((TOKENS,), jnp.float32)
    finals, unused = lax.scan(advance, (lowest, nothing, nothing, lowest, nothing), (teacher_blocks, student_blocks))
    top_teacher, sum_teacher, cross_term, top_student, sum_student = finals
    divergence = cross_term / sum_teacher - top_teacher - jnp.log(sum_teacher) + top_student + jnp.log(sum_student)
    return divergence, jnp.mean(divergence)
```

```python
import jax
import jax.numpy as jnp
from jax import lax
from jax.sharding import Mesh
from jax.sharding import PartitionSpec as P

AXES = ("z", "xh", "core", "xl", "y")
ROW = ("z", "xh", "core")
COL = ("xl", "y")
ROW_COL = ROW + COL
X = ("xh", "xl")

INNER = [(0, 1), (1, 0), (2, 3), (3, 2)]
OUTER = [(1, 2), (2, 1), (3, 0), (0, 3)]
ACROSS = [(0, 2), (2, 0), (1, 3), (3, 1)]
PARTNER = [(0, 1), (1, 0)]


def shift(n, k):
    return [(i, (i + k) % n) for i in range(n)]


def send(x, axis, pairs):
    return lax.ppermute(x, axis, pairs)


def ordered(first, own, other):
    return jnp.where(first, own, other), jnp.where(first, other, own)


def ring(block, half_first, half_second):
    found = {0: block}
    up, down = block, block
    for k in (1, 2, 3):
        up = send(up, "z", shift(8, 1))
        down = send(down, "z", shift(8, -1))
        found[8 - k], found[k] = up, down
    found["4a"] = send(half_first(up), "z", shift(8, 1))
    found["4b"] = send(half_second(down), "z", shift(8, -1))
    return found


def logits(tokens, tables):
    contract = (((1,), (1,)), ((), ()))
    return [lax.dot_general(tokens, t, contract, preferred_element_type=jnp.float32) for t in tables]


def stats(tokens, teacher_tables, student_tables, teacher_width):
    teacher = logits(tokens[:, :teacher_width], teacher_tables)
    student = logits(tokens[:, teacher_width:], student_tables)
    top_teacher = jnp.maximum(jnp.max(teacher[0], 1), jnp.max(teacher[1], 1))
    top_student = jnp.maximum(jnp.max(student[0], 1), jnp.max(student[1], 1))
    sum_teacher = cross_term = sum_student = 0.0
    for t, s in zip(teacher, student):
        weights = jnp.exp(t - top_teacher[:, None])
        sum_teacher += jnp.sum(weights, 1)
        cross_term += jnp.sum(weights * (t - s), 1)
        sum_student += jnp.sum(jnp.exp(s - top_student[:, None]), 1)
    return jnp.stack([top_teacher, sum_teacher, cross_term, top_student, sum_student])


def tree(terms):
    while len(terms) > 1:
        half = len(terms) // 2
        terms = [terms[k] + terms[k + half] for k in range(half)]
    return terms[0]


def merged(parts):
    high_teacher, high_student = parts[0][0], parts[0][3]
    for p in parts[1:]:
        high_teacher, high_student = jnp.maximum(high_teacher, p[0]), jnp.maximum(high_student, p[3])
    teacher = [jnp.exp(p[0] - high_teacher) for p in parts]
    student = [jnp.exp(p[3] - high_student) for p in parts]
    return jnp.stack(
        [
            high_teacher,
            tree([p[1] * f for p, f in zip(parts, teacher)]),
            tree([p[2] * f for p, f in zip(parts, teacher)]),
            high_student,
            tree([p[4] * f for p, f in zip(parts, student)]),
        ]
    )


def per_device(teacher_hidden, student_hidden, teacher_embed, student_embed):
    x = lax.axis_index(X)
    y = lax.axis_index("y")
    count, width = teacher_hidden.shape
    teacher_tables = (teacher_embed, send(teacher_embed, "core", PARTNER))
    student_tables = (student_embed, send(student_embed, "core", PARTNER))
    teacher_width = teacher_embed.shape[1]

    own = jnp.concatenate([teacher_hidden, student_hidden], 1)
    got = send(own, "y", INNER)
    even, odd = ordered(y % 2 == 0, own, got)
    pair = jnp.concatenate([even[:, :width], odd[:, :width], even[:, width:], odd[:, width:]], 1)
    got = send(pair, "y", OUTER)
    low, high = ordered(y < 2, pair, got)
    width = 2 * width
    quad = jnp.concatenate([low[:, :width], high[:, :width], low[:, width:], high[:, width:]], 1)
    width = 2 * width

    def joined(own, other):
        low, high = ordered(x % 2 == 0, own, other)
        return jnp.concatenate([low[:, :width], high[:, :width], low[:, width:], high[:, width:]], 1)

    half = count // 2
    first, second = quad[:half], quad[half:]
    first = joined(first, send(first, X, INNER))
    first = jnp.concatenate([first, send(first, X, OUTER)], 0)
    firsts = ring(first, lambda b: b[:half], lambda b: b[half:])
    seconds = ring(second, lambda b: b[: half // 2], lambda b: b[half // 2 :])
    order = (0, 1, 2, 3, "4a", "4b", 5, 6, 7)
    second = jnp.concatenate([seconds[k] for k in order], 0)
    inner, outer = send(second, X, INNER), send(second, X, OUTER)
    middle = second.shape[0] // 2
    across = jnp.concatenate([send(outer[:middle], X, INNER), send(inner[middle:], X, OUTER)], 0)
    near = joined(second, inner)
    far = joined(across, outer)

    tables = (teacher_tables, student_tables, teacher_width)
    early = stats(jnp.concatenate([firsts[k] for k in (0, 1, 7, 2, 6)], 0), *tables)
    late = stats(jnp.concatenate([firsts[k] for k in (3, 5, "4a", "4b")] + [near, far], 0), *tables)
    early = early.reshape(5, 5, 2, half)
    late_first = late[:, : 6 * half].reshape(5, 3, 2, half)
    near, far = jnp.split(late[:, 6 * half :].reshape(5, 2, 8, 1, half), 2, 1)
    planes = {0: early[:, 0], 1: early[:, 1], 7: early[:, 2], 2: early[:, 3], 6: early[:, 4]}
    planes.update({3: late_first[:, 0], 5: late_first[:, 1], 4: late_first[:, 2]})
    firsts = jnp.stack([planes[k] for k in range(8)], 1)
    seconds = jnp.concatenate([near[:, 0], far[:, 0]], 2)
    current = jnp.concatenate([firsts, seconds], 3)

    current = merged([current] + [send(current, "y", p) for p in (ACROSS, INNER, OUTER)])
    swapped = current[:, :, ::-1]
    current = merged([current, send(swapped, X, ACROSS), send(current, X, INNER), send(swapped, X, OUTER)])
    parts = [current]
    for k in range(1, 8):
        got = send(current, "z", shift(8, k))
        parts.append(jnp.concatenate([got[:, k:], got[:, :k]], 1))
    current = merged(parts)
    top_teacher, sum_teacher, cross_term, top_student, sum_student = current
    divergence = (
        cross_term / sum_teacher - top_teacher - jnp.log(sum_teacher) + top_student + jnp.log(sum_student)
    )
    total = tree([divergence[k, 0] + divergence[k, 1] for k in range(8)])
    total = jnp.sum(total)
    total = total + send(total, "core", PARTNER)
    own_count = count // 8
    own_block = lax.axis_index(COL) * own_count
    mine = lax.dynamic_slice_in_dim(divergence[0, 0], own_block, own_count)
    return mine, total / (count * 32)


def solution(mesh):
    finer = Mesh(mesh.devices.reshape(8, 2, 2, 2, 4), AXES)
    in_specs = (P(ROW, COL), P(ROW, COL), P(ROW_COL, None), P(ROW_COL, None))
    out_specs = (P(ROW_COL), P())
    return jax.shard_map(
        per_device, mesh=finer, in_specs=in_specs, out_specs=out_specs, check_vma=False
    )
```
